128 devices in a mesh: rep: 1, dp: 128 (over x, y, z, core).
Axes of the slice: x: 4, y: 4, z: 4, core: 2. Of those that a mesh axis runs over, the one named last changes fastest.
Arguments:
- x: bfloat16 [128, 1024, 1024], P(('rep', 'dp'))
- dy: bfloat16 [128, 1024, 1024], P(('rep', 'dp'))
- w_gate: bfloat16 [2, 1024, 3328], replicated
- w_up: bfloat16 [2, 1024, 3328], replicated
- w_down: bfloat16 [2, 3328, 1024], replicated
- m_w_gate: float32 [2, 1024, 3328], replicated
- m_w_up: float32 [2, 1024, 3328], replicated
- m_w_down: float32 [2, 3328, 1024], replicated
- v_w_gate: float32 [2, 1024, 3328], replicated
- v_w_up: float32 [2, 1024, 3328], replicated
- v_w_down: float32 [2, 3328, 1024], replicated
Outputs:
- output 1: bfloat16 [2, 1024, 3328], P('rep')
- output 2: bfloat16 [2, 1024, 3328], P('rep')
- output 3: bfloat16 [2, 3328, 1024], P('rep')
- output 4: float32 [2, 1024, 3328], P('rep')
- output 5: float32 [2, 1024, 3328], P('rep')
- output 6: float32 [2, 3328, 1024], P('rep')
- output 7: float32 [2, 1024, 3328], P('rep')
- output 8: float32 [2, 1024, 3328], P('rep')
- output 9: float32 [2, 3328, 1024], P('rep')
All inputs are finite; a program needn't handle non-finite values.
Results may differ from the reference program's by a relative error of at most 0.022.
Values are sent between devices in bfloat16 or wider.
A program may use at most 1.5 GiB of HBM per device.

```python
import jax
import jax.numpy as jnp
from jax import lax

SEQUENCES = 128
TOKENS = 1024
D = 1024
FF = 3328
LAYERS = 2
NAMES = ("w_gate", "w_up", "w_down")
SHAPES = {"w_gate": (LAYERS, D, FF), "w_up": (LAYERS, D, FF), "w_down": (LAYERS, FF, D)}


def bump(key, n, height):
    away = (jnp.arange(n, dtype=jnp.int32) - jax.random.randint(key, (), 0, n, jnp.int32)) % n
    return jnp.where(away < n // 8, height, 1.0)


def together(key, own, strength):
    shared = jax.random.normal(key, own.shape[1:], jnp.float32)
    return (own + strength * shared) * lax.rsqrt(1 + strength * strength)


def setup_inputs(seed: int = 0, part: int = 0) -> dict:
    kx, kdy, ka, kb, kz, kf, kh, kl, *keys = jax.random.split(jax.random.key(seed), 8 + 3 * len(NAMES))
    kx, kdy, ka, kb = (jax.random.fold_in(k, part) for k in (kx, kdy, ka, kb))
    kw, km, kv = (keys[i::3] for i in range(3))
    shape = (SEQUENCES, TOKENS, D)
    much_x, much_dy = jax.random.uniform(kz, (2,), jnp.float32, 0.0, 1.0)
    loud = 2.0 ** jax.random.uniform(jax.random.fold_in(kz, 1), (), jnp.float32, -1.0, 2.0)
    layers = 2.0 ** jax.random.uniform(kl, (LAYERS, 1, 1), jnp.float32, -1.0, 1.0)
    x = together(ka, jax.random.normal(kx, shape, jnp.float32), much_x) * bump(kf, D, 4.0)
    dy = together(kb, jax.random.normal(kdy, shape, jnp.float32), much_dy)
    drawn = {"x": x.astype(jnp.bfloat16), "dy": (loud * dy * (SEQUENCES * TOKENS) ** -0.5).astype(jnp.bfloat16)}
    for key, name in zip(kw, NAMES, strict=True):
        w = jax.random.normal(key, SHAPES[name], jnp.float32) * SHAPES[name][1] ** -0.5
        drawn[name] = (w * {"w_gate": 1.0, "w_up": bump(kh, FF, 4.0), "w_down": layers}[name]).astype(jnp.bfloat16)
    for key, name in zip(km, NAMES, strict=True):
        drawn[f"m_{name}"] = 0.1 * jax.random.normal(key, SHAPES[name], jnp.float32)
    for key, name in zip(kv, NAMES, strict=True):
        drawn[f"v_{name}"] = loud * loud * jax.random.uniform(key, SHAPES[name], jnp.float32, 0.05, 0.15)
    return drawn


def matmul(a, w):
    return jnp.dot(a, w, preferred_element_type=jnp.float32).astype(jnp.bfloat16)


def normed(h):
    wide = h.astype(jnp.float32)
    scale = lax.rsqrt(jnp.mean(wide**2, -1, keepdims=True) + 1e-6)
    return (wide * scale).astype(jnp.bfloat16)


def layer(h, w):
    a = normed(h)
    gate = jnp.dot(a, w["w_gate"], preferred_element_type=jnp.float32)
    up = jnp.dot(a, w["w_up"], preferred_element_type=jnp.float32)
    return h + matmul((jax.nn.silu(gate) * up).astype(jnp.bfloat16), w["w_down"])


def adamw(w, m, v, g):
    m = 0.9 * m + 0.1 * g
    v = 0.95 * v + 0.05 * g * g
    step = m * lax.rsqrt(v + 1e-8) + 0.1 * w
    return (w - 0.02 * step).astype(jnp.bfloat16), m, v


def stack(weights, h):
    return lax.scan(lambda h, w: (layer(h, w), None), h, weights)[0]


def reference(x, dy, w_gate, w_up, w_down, m_w_gate, m_w_up, m_w_down, v_w_gate, v_w_up, v_w_down):
    weights = dict(zip(NAMES, (w_gate, w_up, w_down), strict=True))

    def take(so_far, sequence):
        h, by_y = sequence
        _, back = jax.vjp(lambda w: stack(w, h), weights)
        return jax.tree.map(lambda total, term: total + term.astype(jnp.float32), so_far, back(by_y)[0]), None

    none_yet = {name: jnp.zeros(w.shape, jnp.float32) for name, w in weights.items()}
    by_weights, _ = lax.scan(take, none_yet, (x, dy))
    gradients = [by_weights[name].astype(jnp.bfloat16).astype(jnp.float32) for name in NAMES]
    new = [
        adamw(w.astype(jnp.float32), m, v, g)
        for w, m, v, g in zip((w_gate, w_up, w_down), (m_w_gate, m_w_up, m_w_down), (v_w_gate, v_w_up, v_w_down), gradients, strict=True)
    ]
    return tuple(one[which] for which in range(3) for one in new)
```

```python
import functools

import jax
import jax.numpy as jnp
from jax import lax
from jax.experimental import pallas as pl
from jax.experimental.pallas import tpu as pltpu
from jax.sharding import PartitionSpec as P

NAMES = ("w_gate", "w_up", "w_down")
MESH = pl.DeviceIdType.MESH
SIDE = 4
STRIDE = (32, 8, 2)
OFFSETS = (2, 1, 3)
D, FF, TOKENS = 1024, 3328, 1024
HALF = FF // 2
SLOTS = 4


def matmul(a, w):
    return jnp.dot(a, w, preferred_element_type=jnp.float32).astype(jnp.bfloat16)


def matmul_t(a, w):
    return lax.dot_general(a, w, (((1,), (1,)), ((), ())), preferred_element_type=jnp.float32).astype(jnp.bfloat16)


def normed(h):
    wide = h.astype(jnp.float32)
    scale = lax.rsqrt(jnp.mean(wide**2, -1, keepdims=True) + 1e-6)
    return (wide * scale).astype(jnp.bfloat16)


def exchange_kernel(l0, l1, l2, r0, r1, r2, out, lhs, rhs, mine, part, got_a, got_b, got_c, total, load, core_s, core_r, a_s, a_r, b_s, b_r, c_s, c_r):
    me = lax.axis_index("dp")
    core = lax.rem(me, 2)
    partner = me + 1 - 2 * core
    place = [lax.rem(lax.div(me, s), SIDE) for s in STRIDE]

    def to(device):
        return {"device_id": (0, device), "device_id_type": MESH}

    def along(axis, k):
        there = lax.rem(place[axis] + k, SIDE)
        return me + (there - place[axis]) * STRIDE[axis], there

    loads = []
    for n, (src, dst) in enumerate([(l2, lhs.at[2]), (r2, rhs.at[2]), (l0, lhs.at[0]), (r0, rhs.at[0]), (l1, lhs.at[1]), (r1, rhs.at[1])]):
        copy = pltpu.make_async_copy(src, dst, load.at[n])
        copy.start()
        loads.append(copy)
    barrier = pltpu.get_barrier_semaphore()
    pl.semaphore_signal(barrier, inc=1, **to(partner))
    for axis in range(3):
        for k in OFFSETS:
            pl.semaphore_signal(barrier, inc=1, **to(along(axis, k)[0]))
    pl.semaphore_wait(barrier, 10)

    def rows(index, size):
        return pl.ds(pl.multiple_of(index * size, size), size)

    order = (2, 0, 1)
    units = [(m, step) for step in range(4) for m in order]

    def block_of(m, step):
        return along(m, OFFSETS[step])[1] if step < 3 else place[m]

    def product(m, block, half):
        columns = pl.ds(pl.multiple_of(half * HALF, 128), HALF)
        return jnp.dot(lhs[m, rows(block, 256), :], rhs[m, :, columns], preferred_element_type=jnp.float32)

    core_copies, sends = [], []

    def give(n):
        m, step = units[n]
        if step == 0:
            loads[2 * order.index(m)].wait()
            loads[2 * order.index(m) + 1].wait()
        slot = n % SLOTS
        if n >= SLOTS:
            core_copies[n - SLOTS].wait_send()
        mine[slot] = product(m, block_of(m, step), 1 - core).astype(jnp.bfloat16)
        copy = pltpu.make_async_remote_copy(mine.at[slot], part.at[n], core_s.at[n], core_r.at[n], **to(partner))
        copy.start()
        core_copies.append(copy)

    ahead = 3
    for n in range(ahead):
        give(n)
    for n, (m, step) in enumerate(units):
        if n + ahead < len(units):
            give(n + ahead)
        own = product(m, block_of(m, step), core)
        core_copies[n].wait_recv()
        summed = own + part[n].astype(jnp.float32)
        if step < 3:
            part[n] = summed.astype(jnp.bfloat16)
            copy = pltpu.make_async_remote_copy(part.at[n], got_a.at[m, step], a_s.at[m, step], a_r.at[m, step], **to(along(m, OFFSETS[step])[0]))
            copy.start()
            sends.append((m, copy))
        else:
            total[m] = summed

    def level(axis_of, got_from, copies, size, buffer, got, s, r):
        following = []
        for m in order:
            for n, copy in copies:
                if n == m:
                    copy.wait_recv()
            summed = total[m, : 4 * size]
            for step in range(3):
                summed = summed + got_from[m, step].astype(jnp.float32)
            total[m, : 4 * size] = summed
            buffer[m] = summed.astype(jnp.bfloat16)
            axis = axis_of(m)
            for step in range(3):
                device, there = along(axis, OFFSETS[step])
                copy = pltpu.make_async_remote_copy(buffer.at[m, rows(there, size)], got.at[m, step], s.at[m, step], r.at[m, step], **to(device))
                copy.start()
                following.append((m, copy))
            kept = total[m, rows(place[axis], size), :]
            total[m, :size] = kept
        return following

    def second(m):
        return (m + 1) % 3

    def third(m):
        return (m + 2) % 3

    b_copies = level(second, got_a, sends, 64, got_b["send"], got_b["got"], b_s, b_r)
    c_copies = level(third, got_b["got"], b_copies, 16, got_c["send"], got_c["got"], c_s, c_r)
    for m in order:
        for n, copy in c_copies:
            if n == m:
                copy.wait_recv()
        summed = total[m, :16]
        for step in range(3):
            summed = summed + got_c["got"][m, step].astype(jnp.float32)
        out[:, m * HALF : (m + 1) * HALF] = summed.astype(jnp.bfloat16)
    for copy in core_copies[-SLOTS:]:
        copy.wait_send()
    for _, copy in sends + b_copies + c_copies:
        copy.wait_send()


def exchange(lhs, rhs, number):
    def dma(*shape):
        return pltpu.SemaphoreType.DMA(shape)

    bf16, f32 = jnp.bfloat16, jnp.float32
    return pl.pallas_call(
        exchange_kernel,
        out_shape=jax.ShapeDtypeStruct((16, 3 * HALF), bf16),
        in_specs=[pl.BlockSpec(memory_space=pl.ANY)] * 6,
        out_specs=pl.BlockSpec(memory_space=pltpu.VMEM),
        scratch_shapes=[
            pltpu.VMEM((3, D, TOKENS), bf16),
            pltpu.VMEM((3, TOKENS, FF), bf16),
            pltpu.VMEM((SLOTS, 256, HALF), bf16),
            pltpu.VMEM((12, 256, HALF), bf16),
            pltpu.VMEM((3, 3, 256, HALF), bf16),
            {"send": pltpu.VMEM((3, 256, HALF), bf16), "got": pltpu.VMEM((3, 3, 64, HALF), bf16)},
            {"send": pltpu.VMEM((3, 64, HALF), bf16), "got": pltpu.VMEM((3, 3, 16, HALF), bf16)},
            pltpu.VMEM((3, 256, HALF), f32),
            dma(6),
            dma(12),
            dma(12),
            *[dma(3, 3)] * 6,
        ],
        compiler_params=pltpu.CompilerParams(collective_id=number, has_side_effects=True, vmem_limit_bytes=67_043_328),
        cost_estimate=pl.CostEstimate(flops=6 * D * TOKENS * FF, bytes_accessed=26_000_000, transcendentals=0),
        name=f"exchange_{number}",
    )(*lhs, *rhs)


def update(w, m, v, g):
    m = 0.9 * m + 0.1 * g
    v = 0.95 * v + 0.05 * g * g
    step = m * lax.rsqrt(v + 1e-8) + 0.1 * w
    return w - 0.02 * step, m, v


def adamw_kernel(g, w, m, v, *rest):
    new_w, new_m, new_v = rest[-3:]
    for half in range(2):
        at = (0, slice(None), slice(half * HALF, (half + 1) * HALF))
        one = g[:, half].reshape(w.shape[1], HALF).astype(jnp.float32)
        a, b, c = update(w[at].astype(jnp.float32), m[at], v[at], one)
        new_w[at] = a.astype(jnp.bfloat16)
        new_m[at] = b
        new_v[at] = c


def adamw_down_kernel(g, w, m, v, *rest):
    new_w, new_m, new_v = rest[-3:]
    one = g[:, 0].reshape(D, 128).astype(jnp.float32).T
    a, b, c = update(w[0].astype(jnp.float32), m[0], v[0], one)
    new_w[0] = a.astype(jnp.bfloat16)
    new_m[0] = b
    new_v[0] = c


def adamw(which, layer, gathered, w, m, v, before):
    if which < 2:
        size = 64
        body, steps = adamw_kernel, D // size
        g_spec = pl.BlockSpec((size // 16, 2, 16, HALF), lambda i: (i, 0, 0, which))
        spec = pl.BlockSpec((1, size, FF), lambda i: (layer, i, 0))
    else:
        body, steps = adamw_down_kernel, FF // 128
        g_spec = pl.BlockSpec((64, 1, 16, 128), lambda i: (0, i // 13, 0, 26 + i % 13))
        spec = pl.BlockSpec((1, 128, D), lambda i: (layer, i, 0))
    more = [] if before is None else list(before)
    shapes = [jax.ShapeDtypeStruct(w.shape, t) for t in (jnp.bfloat16, jnp.float32, jnp.float32)]
    return pl.pallas_call(
        body,
        grid=(steps,),
        out_shape=shapes,
        in_specs=[g_spec, spec, spec, spec] + [pl.BlockSpec(memory_space=pl.ANY)] * len(more),
        out_specs=[spec] * 3,
        input_output_aliases={4 + i: i for i in range(len(more))},
        compiler_params=pltpu.CompilerParams(vmem_limit_bytes=50_000_000),
        cost_estimate=pl.CostEstimate(flops=20 * D * FF, bytes_accessed=22 * D * FF, transcendentals=D * FF),
        name=f"adamw_{which}_{layer}",
    )(gathered, w, m, v, *more)


def by_owner(t, first):
    blocks = t.reshape(SIDE, SIDE, SIDE, 16, t.shape[1])
    order = [(first + i) % 3 for i in range(3)]
    return blocks.transpose(*order, 3, 4).reshape(t.shape)


def solution(mesh):
    def step(x, dy, *arrays):
        weights, m, v = (arrays[i : i + 3] for i in (0, 3, 6))
        layers = weights[0].shape[0]
        w_gate, w_up, w_down = weights
        h, kept = x[0], []
        for n in range(layers):
            a, back = jax.vjp(normed, h)
            gate = jnp.dot(a, w_gate[n], preferred_element_type=jnp.float32)
            up = jnp.dot(a, w_up[n], preferred_element_type=jnp.float32)
            hidden = (jax.nn.silu(gate) * up).astype(jnp.bfloat16)
            kept.append((a, back, gate, up, hidden))
            if n < layers - 1:
                h = h + matmul(hidden, w_down[n])
        by_h, gathered = dy[0], [None] * layers
        for n in reversed(range(layers)):
            a, back, gate, up, hidden = kept[n]
            by_hidden = matmul_t(by_h, w_down[n]).astype(jnp.float32)
            sig = jax.nn.sigmoid(gate)
            silu = gate * sig
            by_up = (by_hidden * silu).astype(jnp.bfloat16)
            by_gate = (by_hidden * up * (sig + silu * (1 - sig))).astype(jnp.bfloat16)
            a_t, by_h_t = a.T, by_h.T
            lhs = [by_owner(a_t, 0), by_owner(a_t, 1), by_owner(by_h_t, 2)]
            chunk = exchange(lhs, [by_gate, by_up, hidden], n)
            gathered[n] = lax.all_gather(chunk, "dp", axis=0, tiled=False).reshape(64, 2, 16, 3 * HALF)
            if n:
                (by_in,) = back(matmul_t(by_gate, w_gate[n]) + matmul_t(by_up, w_up[n]))
                by_h = by_h + by_in
        new = [None] * 3
        for n in reversed(range(layers)):
            new = [adamw(i, n, gathered[n], weights[i], m[i], v[i], new[i]) for i in range(3)]
        return tuple(one[which] for which in range(3) for one in new)

    return jax.shard_map(
        step,
        mesh=mesh,
        in_specs=(P(("rep", "dp"), None, None),) * 2 + (P(None, None, None),) * 9,
        out_specs=(P("rep", None, None),) * 9,
        check_vma=False,
    )
```

```python
import jax
import jax.numpy as jnp
from jax import lax
from jax.experimental import pallas as pl
from jax.experimental.pallas import tpu as pltpu
from jax.sharding import PartitionSpec as P

NAMES = ("w_gate", "w_up", "w_down")
MESH = pl.DeviceIdType.MESH
SIDE = 4
STRIDE = (32, 8, 2)
OFFSETS = (2, 1, 3)
D, FF, TOKENS = 1024, 3328, 1024
HALF = FF // 2
SLOTS = 4


def scale_of(wide):
    return lax.rsqrt(jnp.mean(wide**2, -1, keepdims=True) + 1e-6)


def normed(h):
    wide = h.astype(jnp.float32)
    return (wide * scale_of(wide)).astype(jnp.bfloat16)


def dot(a, w):
    return jnp.dot(a, w, preferred_element_type=jnp.float32)


def dot_t(a, w):
    return lax.dot_general(a, w, (((1,), (1,)), ((), ())), preferred_element_type=jnp.float32)


def add_up(total, term):
    first = pl.program_id(0) == 0

    @pl.when(first)
    def _():
        total[...] = term

    @pl.when(jnp.logical_not(first))
    def _():
        total[...] += term


def last():
    return pl.program_id(0) == pl.num_programs(0) - 1


def forward_kernel(h, a, w_gate, w_up, w_down, gate, up, hidden, next_h, next_a, total):
    gate[...] = dot(a[...], w_gate[0])
    up[...] = dot(a[...], w_up[0])
    hidden[...] = (jax.nn.silu(gate[...]) * up[...]).astype(jnp.bfloat16)
    add_up(total, dot(hidden[...], w_down[0]))

    @pl.when(last())
    def _():
        out = h[...] + total[...].astype(jnp.bfloat16)
        next_h[...] = out
        next_a[...] = normed(out)


def by_gate_and_up(gate, up, by_hidden):
    by_hidden = by_hidden.astype(jnp.bfloat16).astype(jnp.float32)
    sig = jax.nn.sigmoid(gate)
    silu = gate * sig
    by_up = (by_hidden * silu).astype(jnp.bfloat16)
    by_gate = (by_hidden * up * (sig + silu * (1 - sig))).astype(jnp.bfloat16)
    return silu, by_gate, by_up


def last_layer_kernel(by_h, a, w_gate, w_up, w_down, hidden, by_gate, by_up):
    gate, up = dot(a[...], w_gate[0]), dot(a[...], w_up[0])
    silu, by_gate[...], by_up[...] = by_gate_and_up(gate, up, dot_t(by_h[...], w_down[0]))
    hidden[...] = (silu * up).astype(jnp.bfloat16)


def backward_kernel(by_h, w_down, gate, up, by_gate, by_up):
    _, by_gate[...], by_up[...] = by_gate_and_up(gate[...], up[...], dot_t(by_h[...], w_down[0]))


def by_input_kernel(h, by_h, by_gate, by_up, w_gate, w_up, by_in, total_gate, total_up):
    add_up(total_gate, dot_t(by_gate[...], w_gate[0]))
    add_up(total_up, dot_t(by_up[...], w_up[0]))

    @pl.when(last())
    def _():
        by_a = (total_gate[...].astype(jnp.bfloat16) + total_up[...].astype(jnp.bfloat16)).astype(jnp.float32)
        wide = h[...].astype(jnp.float32)
        scale = scale_of(wide)
        shared = jnp.sum(by_a * wide, -1, keepdims=True) * scale**3 / D
        by_in[...] = by_h[...] + (by_a * scale - wide * shared).astype(jnp.bfloat16)


TILE = 256


def over_hidden(body, name, layer, kinds, out_kinds, totals, matmuls, *args):
    specs = {
        "s": pl.BlockSpec((TOKENS, D), lambda j: (0, 0)),
        "r": pl.BlockSpec((1, TILE, D), lambda j: (layer, j, 0)),
        "c": pl.BlockSpec((1, D, TILE), lambda j: (layer, 0, j)),
        "t": pl.BlockSpec((TOKENS, TILE), lambda j: (0, j)),
        "f": pl.BlockSpec((TOKENS, TILE), lambda j: (0, j)),
    }
    shapes = {
        "s": jax.ShapeDtypeStruct((TOKENS, D), jnp.bfloat16),
        "t": jax.ShapeDtypeStruct((TOKENS, FF), jnp.bfloat16),
        "f": jax.ShapeDtypeStruct((TOKENS, FF), jnp.float32),
    }
    return pl.pallas_call(
        body,
        grid=(FF // TILE,),
        in_specs=[specs[k] for k in kinds],
        out_specs=[specs[k] for k in out_kinds],
        out_shape=[shapes[k] for k in out_kinds],
        scratch_shapes=[pltpu.VMEM((TOKENS, D), jnp.float32)] * totals,
        compiler_params=pltpu.CompilerParams(vmem_limit_bytes=60_000_000),
        cost_estimate=pl.CostEstimate(flops=2 * matmuls * TOKENS * D * FF, bytes_accessed=40_000_000, transcendentals=TOKENS * FF),
        name=name,
    )(*args)


def exchange_kernel(l0, l1, l2, r0, r1, r2, out, lhs, rhs, mine, part, got_a, got_b, got_c, total, load, core_s, core_r, a_s, a_r, b_s, b_r, c_s, c_r):
    me = lax.axis_index("dp")
    core = lax.rem(me, 2)
    partner = me + 1 - 2 * core
    place = [lax.rem(lax.div(me, s), SIDE) for s in STRIDE]

    def to(device):
        return {"device_id": (0, device), "device_id_type": MESH}

    def along(axis, k):
        there = lax.rem(place[axis] + k, SIDE)
        return me + (there - place[axis]) * STRIDE[axis], there

    loads = []
    for n, (src, dst) in enumerate([(l2, lhs.at[2]), (r2, rhs.at[2]), (l0, lhs.at[0]), (r0, rhs.at[0]), (l1, lhs.at[1]), (r1, rhs.at[1])]):
        copy = pltpu.make_async_copy(src, dst, load.at[n])
        copy.start()
        loads.append(copy)
    barrier = pltpu.get_barrier_semaphore()
    pl.semaphore_signal(barrier, inc=1, **to(partner))
    for axis in range(3):
        for k in OFFSETS:
            pl.semaphore_signal(barrier, inc=1, **to(along(axis, k)[0]))
    pl.semaphore_wait(barrier, 10)

    def rows(index, size):
        return pl.ds(pl.multiple_of(index * size, size), size)

    order = (2, 0, 1)
    units = [(m, step) for step in range(4) for m in order]

    def block_of(m, step):
        return along(m, OFFSETS[step])[1] if step < 3 else place[m]

    def product(m, block, half):
        columns = pl.ds(pl.multiple_of(half * HALF, 128), HALF)
        return jnp.dot(lhs[m, rows(block, 256), :], rhs[m, :, columns], preferred_element_type=jnp.float32)

    core_copies, sends = [], []

    def give(n):
        m, step = units[n]
        if step == 0:
            loads[2 * order.index(m)].wait()
            loads[2 * order.index(m) + 1].wait()
        slot = n % SLOTS
        if n >= SLOTS:
            core_copies[n - SLOTS].wait_send()
        mine[slot] = product(m, block_of(m, step), 1 - core).astype(jnp.bfloat16)
        copy = pltpu.make_async_remote_copy(mine.at[slot], part.at[n], core_s.at[n], core_r.at[n], **to(partner))
        copy.start()
        core_copies.append(copy)

    ahead = 3
    for n in range(ahead):
        give(n)
    for n, (m, step) in enumerate(units):
        if n + ahead < len(units):
            give(n + ahead)
        own = product(m, block_of(m, step), core)
        core_copies[n].wait_recv()
        summed = own + part[n].astype(jnp.float32)
        if step < 3:
            part[n] = summed.astype(jnp.bfloat16)
            copy = pltpu.make_async_remote_copy(part.at[n], got_a.at[m, step], a_s.at[m, step], a_r.at[m, step], **to(along(m, OFFSETS[step])[0]))
            copy.start()
            sends.append((m, copy))
        else:
            total[m] = summed

    def level(axis_of, got_from, copies, size, buffer, got, s, r):
        following = []
        for m in order:
            for n, copy in copies:
                if n == m:
                    copy.wait_recv()
            summed = total[m, : 4 * size]
            for step in range(3):
                summed = summed + got_from[m, step].astype(jnp.float32)
            total[m, : 4 * size] = summed
            buffer[m] = summed.astype(jnp.bfloat16)
            axis = axis_of(m)
            for step in range(3):
                device, there = along(axis, OFFSETS[step])
                copy = pltpu.make_async_remote_copy(buffer.at[m, rows(there, size)], got.at[m, step], s.at[m, step], r.at[m, step], **to(device))
                copy.start()
                following.append((m, copy))
            kept = total[m, rows(place[axis], size), :]
            total[m, :size] = kept
        return following

    def second(m):
        return (m + 1) % 3

    def third(m):
        return (m + 2) % 3

    b_copies = level(second, got_a, sends, 64, got_b["send"], got_b["got"], b_s, b_r)
    c_copies = level(third, got_b["got"], b_copies, 16, got_c["send"], got_c["got"], c_s, c_r)
    for m in order:
        for n, copy in c_copies:
            if n == m:
                copy.wait_recv()
        summed = total[m, :16]
        for step in range(3):
            summed = summed + got_c["got"][m, step].astype(jnp.float32)
        out[:, m * HALF : (m + 1) * HALF] = summed.astype(jnp.bfloat16)
    for copy in core_copies[-SLOTS:]:
        copy.wait_send()
    for _, copy in sends + b_copies + c_copies:
        copy.wait_send()


def exchange(lhs, rhs, number):
    def dma(*shape):
        return pltpu.SemaphoreType.DMA(shape)

    bf16, f32 = jnp.bfloat16, jnp.float32
    return pl.pallas_call(
        exchange_kernel,
        out_shape=jax.ShapeDtypeStruct((16, 3 * HALF), bf16),
        in_specs=[pl.BlockSpec(memory_space=pl.ANY)] * 6,
        out_specs=pl.BlockSpec(memory_space=pltpu.VMEM),
        scratch_shapes=[
            pltpu.VMEM((3, D, TOKENS), bf16),
            pltpu.VMEM((3, TOKENS, FF), bf16),
            pltpu.VMEM((SLOTS, 256, HALF), bf16),
            pltpu.VMEM((12, 256, HALF), bf16),
            pltpu.VMEM((3, 3, 256, HALF), bf16),
            {"send": pltpu.VMEM((3, 256, HALF), bf16), "got": pltpu.VMEM((3, 3, 64, HALF), bf16)},
            {"send": pltpu.VMEM((3, 64, HALF), bf16), "got": pltpu.VMEM((3, 3, 16, HALF), bf16)},
            pltpu.VMEM((3, 256, HALF), f32),
            dma(6),
            dma(12),
            dma(12),
            *[dma(3, 3)] * 6,
        ],
        compiler_params=pltpu.CompilerParams(collective_id=number, has_side_effects=True, vmem_limit_bytes=67_043_328),
        cost_estimate=pl.CostEstimate(flops=6 * D * TOKENS * FF, bytes_accessed=26_000_000, transcendentals=0),
        name=f"exchange_{number}",
    )(*lhs, *rhs)


def update(w, m, v, g):
    m = 0.9 * m + 0.1 * g
    v = 0.95 * v + 0.05 * g * g
    step = m * lax.rsqrt(v + 1e-8) + 0.1 * w
    return w - 0.02 * step, m, v


ROWS = 64
STEPS = (D // ROWS, D // ROWS, FF // 128)


def adamw_kernel(*refs):
    g, w, m, v = (refs[i : i + 3] for i in (0, 3, 6, 9))
    new_w, new_m, new_v = refs[-9:-6], refs[-6:-3], refs[-3:]
    i = pl.program_id(0)
    start = 0
    for n in range(3):

        @pl.when((i >= start) & (i < start + STEPS[n]))
        def _(n=n):
            if n < 2:
                parts = [(slice(half * HALF, (half + 1) * HALF), g[n][:, half].reshape(ROWS, HALF)) for half in range(2)]
            else:
                parts = [(slice(None), g[n][:, 0].reshape(D, 128).T)]
            for columns, one in parts:
                at = (0, slice(None), columns)
                a, b, c = update(w[n][at].astype(jnp.float32), m[n][at], v[n][at], one.astype(jnp.float32))
                new_w[n][at] = a.astype(jnp.bfloat16)
                new_m[n][at] = b
                new_v[n][at] = c

        start += STEPS[n]


def adamw(layer, gathered, w, m, v, before):
    def at(n):
        start = sum(STEPS[:n])
        return lambda i: jnp.clip(i - start, 0, STEPS[n] - 1)

    def down(i):
        i = at(2)(i)
        return 0, i // 13, 0, 26 + i % 13

    g_specs = [pl.BlockSpec((ROWS // 16, 2, 16, HALF), lambda i, n=n: (at(n)(i), 0, 0, n)) for n in range(2)]
    g_specs.append(pl.BlockSpec((64, 1, 16, 128), down))
    specs = [pl.BlockSpec((1, ROWS, FF), lambda i, n=n: (layer, at(n)(i), 0)) for n in range(2)]
    specs.append(pl.BlockSpec((1, 128, D), lambda i: (layer, at(2)(i), 0)))
    more = [] if before is None else list(before)
    shapes = [jax.ShapeDtypeStruct(one.shape, t) for t in (jnp.bfloat16, jnp.float32, jnp.float32) for one in w]
    return pl.pallas_call(
        adamw_kernel,
        grid=(sum(STEPS),),
        out_shape=shapes,
        in_specs=g_specs + specs * 3 + [pl.BlockSpec(memory_space=pl.ANY)] * len(more),
        out_specs=specs * 3,
        input_output_aliases={12 + i: i for i in range(len(more))},
        compiler_params=pltpu.CompilerParams(vmem_limit_bytes=60_000_000),
        cost_estimate=pl.CostEstimate(flops=60 * D * FF, bytes_accessed=66 * D * FF, transcendentals=3 * D * FF),
        name=f"adamw_{layer}",
    )(gathered, gathered, gathered, *w, *m, *v, *more)


def by_owner(t, first):
    blocks = t.reshape(SIDE, SIDE, SIDE, 16, t.shape[1])
    order = [(first + i) % 3 for i in range(3)]
    return blocks.transpose(*order, 3, 4).reshape(t.shape)


def solution(mesh):
    def step(x, dy, *arrays):
        weights, m, v = (arrays[i : i + 3] for i in (0, 3, 6))
        w_gate, w_up, w_down = weights
        states, by_y = x[0], dy[0]
        a = normed(states)
        gate, up, hidden, middle, b = over_hidden(forward_kernel, "forward", 0, "ssccr", "fftss", 1, 3, states, a, w_gate, w_up, w_down)
        last_hidden, by_gate, by_up = over_hidden(last_layer_kernel, "last_layer", 1, "ssccr", "ttt", 0, 3, by_y, b, w_gate, w_up, w_down)

        def sums(number, a, by_h, by_gate, by_up, hidden):
            a_t = a.T
            lhs = [by_owner(a_t, 0), by_owner(a_t, 1), by_owner(by_h.T, 2)]
            chunk = exchange(lhs, [by_gate, by_up, hidden], number)
            return lax.all_gather(chunk, "dp", axis=0, tiled=False).reshape(64, 2, 16, 3 * HALF)

        gathered = [None, sums(1, b, by_y, by_gate, by_up, last_hidden)]
        (by_middle,) = over_hidden(by_input_kernel, "by_input", 1, "ssttcc", "s", 2, 2, middle, by_y, by_gate, by_up, w_gate, w_up)
        by_gate, by_up = over_hidden(backward_kernel, "backward", 0, "srff", "tt", 0, 1, by_middle, w_down, gate, up)
        gathered[0] = sums(0, a, by_middle, by_gate, by_up, hidden)
        new = None
        for n in (1, 0):
            new = adamw(n, gathered[n], weights, m, v, new)
        return tuple(new)

    return jax.shard_map(
        step,
        mesh=mesh,
        in_specs=(P(("rep", "dp"), None, None),) * 2 + (P(None, None, None),) * 9,
        out_specs=(P("rep", None, None),) * 9,
        check_vma=False,
    )
```

```python
import jax
import jax.numpy as jnp
from jax import lax
from jax.experimental import pallas as pl
from jax.experimental.pallas import tpu as pltpu
from jax.sharding import PartitionSpec as P

NAMES = ("w_gate", "w_up", "w_down")
MESH = pl.DeviceIdType.MESH
SIDE = 4
STRIDE = (32, 8, 2)
OFFSETS = (2, 1, 3)
D, FF, TOKENS = 1024, 3328, 1024
HALF = FF // 2
SLOTS = 4


def scale_of(wide):
    return lax.rsqrt(jnp.mean(wide**2, -1, keepdims=True) + 1e-6)


def normed(h):
    wide = h.astype(jnp.float32)
    return (wide * scale_of(wide)).astype(jnp.bfloat16)


def dot(a, w):
    return jnp.dot(a, w, preferred_element_type=jnp.float32)


def dot_t(a, w):
    return lax.dot_general(a, w, (((1,), (1,)), ((), ())), preferred_element_type=jnp.float32)


def add_up(total, term):
    first = pl.program_id(0) == 0

    @pl.when(first)
    def _():
        total[...] = term

    @pl.when(jnp.logical_not(first))
    def _():
        total[...] += term


def last():
    return pl.program_id(0) == pl.num_programs(0) - 1


def forward_kernel(h, w_gate, w_up, w_down, gate, up, hidden, a, next_h, next_a, total):
    @pl.when(pl.program_id(0) == 0)
    def _():
        a[...] = normed(h[...])

    gate[...] = dot(a[...], w_gate[0])
    up[...] = dot(a[...], w_up[0])
    hidden[...] = (jax.nn.silu(gate[...]) * up[...]).astype(jnp.bfloat16)
    add_up(total, dot(hidden[...], w_down[0]))

    @pl.when(last())
    def _():
        out = h[...] + total[...].astype(jnp.bfloat16)
        next_h[...] = out
        next_a[...] = normed(out)


def by_gate_and_up(gate, up, by_hidden):
    by_hidden = by_hidden.astype(jnp.bfloat16).astype(jnp.float32)
    sig = jax.nn.sigmoid(gate)
    silu = gate * sig
    by_up = (by_hidden * silu).astype(jnp.bfloat16)
    by_gate = (by_hidden * up * (sig + silu * (1 - sig))).astype(jnp.bfloat16)
    return silu, by_gate, by_up


def last_layer_kernel(by_h, a, w_gate, w_up, w_down, hidden, by_gate, by_up):
    gate, up = dot(a[...], w_gate[0]), dot(a[...], w_up[0])
    silu, by_gate[...], by_up[...] = by_gate_and_up(gate, up, dot_t(by_h[...], w_down[0]))
    hidden[...] = (silu * up).astype(jnp.bfloat16)


def matmul_t(a, w):
    return dot_t(a, w).astype(jnp.bfloat16)


TILE = 256


def over_hidden(body, name, layer, kinds, out_kinds, totals, matmuls, *args):
    specs = {
        "s": pl.BlockSpec((TOKENS, D), lambda j: (0, 0)),
        "r": pl.BlockSpec((1, TILE, D), lambda j: (layer, j, 0)),
        "c": pl.BlockSpec((1, D, TILE), lambda j: (layer, 0, j)),
        "t": pl.BlockSpec((TOKENS, TILE), lambda j: (0, j)),
        "f": pl.BlockSpec((TOKENS, TILE), lambda j: (0, j)),
    }
    shapes = {
        "s": jax.ShapeDtypeStruct((TOKENS, D), jnp.bfloat16),
        "t": jax.ShapeDtypeStruct((TOKENS, FF), jnp.bfloat16),
        "f": jax.ShapeDtypeStruct((TOKENS, FF), jnp.float32),
    }
    return pl.pallas_call(
        body,
        grid=(FF // TILE,),
        in_specs=[specs[k] for k in kinds],
        out_specs=[specs[k] for k in out_kinds],
        out_shape=[shapes[k] for k in out_kinds],
        scratch_shapes=[pltpu.VMEM((TOKENS, D), jnp.float32)] * totals,
        compiler_params=pltpu.CompilerParams(vmem_limit_bytes=60_000_000),
        cost_estimate=pl.CostEstimate(flops=2 * matmuls * TOKENS * D * FF, bytes_accessed=40_000_000, transcendentals=TOKENS * FF),
        name=name,
    )(*args)


def exchange_kernel(a, by_h, r0, r1, r2, out, lhs, rhs, mine, part, got_a, got_b, got_c, total, load, core_s, core_r, a_s, a_r, b_s, b_r, c_s, c_r):
    me = lax.axis_index("dp")
    core = lax.rem(me, 2)
    partner = me + 1 - 2 * core
    place = [lax.rem(lax.div(me, s), SIDE) for s in STRIDE]

    def to(device):
        return {"device_id": (0, device), "device_id_type": MESH}

    def along(axis, k):
        there = lax.rem(place[axis] + k, SIDE)
        return me + (there - place[axis]) * STRIDE[axis], there

    order = (2, 0, 1)
    states = []
    for n, (src, dst) in enumerate(((by_h, part), (a, mine))):
        for quarter in range(4):
            copy = pltpu.make_async_copy(src.at[pl.ds(256 * quarter, 256)], dst.at[quarter, :, pl.ds(0, D)], load.at[4 * n + quarter])
            copy.start()
            states.append(copy)
    loads = {}
    for m in order:
        loads[m] = pltpu.make_async_copy((r0, r1, r2)[m], rhs.at[m], load.at[8 + m])
        loads[m].start()
    for n, (held, products) in enumerate(((part, (2,)), (mine, (0, 1)))):
        for quarter in range(4):
            states[4 * n + quarter].wait()
            for block in range(D // 128):
                turned = held[quarter, :, 128 * block : 128 * (block + 1)].T
                for i in range(8):
                    at = (block // 2, 2 * (block % 2) + i // 4, i % 4)
                    for m in products:
                        row = 16 * (16 * at[m] + 4 * at[(m + 1) % 3] + at[(m + 2) % 3])
                        lhs[m, row : row + 16, 256 * quarter : 256 * (quarter + 1)] = turned[16 * i : 16 * (i + 1)]
    barrier = pltpu.get_barrier_semaphore()
    pl.semaphore_signal(barrier, inc=1, **to(partner))
    for axis in range(3):
        for k in OFFSETS:
            pl.semaphore_signal(barrier, inc=1, **to(along(axis, k)[0]))
    pl.semaphore_wait(barrier, 10)

    def rows(index, size):
        return pl.ds(pl.multiple_of(index * size, size), size)

    units = [(m, step) for step in range(4) for m in order]

    def block_of(m, step):
        return along(m, OFFSETS[step])[1] if step < 3 else place[m]

    def product(m, block, half):
        columns = pl.ds(pl.multiple_of(half * HALF, 128), HALF)
        return jnp.dot(lhs[m, rows(block, 256), :], rhs[m, :, columns], preferred_element_type=jnp.float32)

    core_copies, sends = [], []

    def give(n):
        m, step = units[n]
        if step == 0:
            loads[m].wait()
        slot = n % SLOTS
        if n >= SLOTS:
            core_copies[n - SLOTS].wait_send()
        mine[slot] = product(m, block_of(m, step), 1 - core).astype(jnp.bfloat16)
        copy = pltpu.make_async_remote_copy(mine.at[slot], part.at[n], core_s.at[n], core_r.at[n], **to(partner))
        copy.start()
        core_copies.append(copy)

    ahead = 3
    for n in range(ahead):
        give(n)
    for n, (m, step) in enumerate(units):
        if n + ahead < len(units):
            give(n + ahead)
        own = product(m, block_of(m, step), core)
        core_copies[n].wait_recv()
        summed = own + part[n].astype(jnp.float32)
        if step < 3:
            part[n] = summed.astype(jnp.bfloat16)
            copy = pltpu.make_async_remote_copy(part.at[n], got_a.at[m, step], a_s.at[m, step], a_r.at[m, step], **to(along(m, OFFSETS[step])[0]))
            copy.start()
            sends.append((m, copy))
        else:
            total[m] = summed

    def level(axis_of, got_from, copies, size, buffer, got, s, r):
        following = []
        for m in order:
            for n, copy in copies:
                if n == m:
                    copy.wait_recv()
            summed = total[m, : 4 * size]
            for step in range(3):
                summed = summed + got_from[m, step].astype(jnp.float32)
            total[m, : 4 * size] = summed
            buffer[m] = summed.astype(jnp.bfloat16)
            axis = axis_of(m)
            for step in range(3):
                device, there = along(axis, OFFSETS[step])
                copy = pltpu.make_async_remote_copy(buffer.at[m, rows(there, size)], got.at[m, step], s.at[m, step], r.at[m, step], **to(device))
                copy.start()
                following.append((m, copy))
            kept = total[m, rows(place[axis], size), :]
            total[m, :size] = kept
        return following

    def second(m):
        return (m + 1) % 3

    def third(m):
        return (m + 2) % 3

    b_copies = level(second, got_a, sends, 64, got_b["send"], got_b["got"], b_s, b_r)
    c_copies = level(third, got_b["got"], b_copies, 16, got_c["send"], got_c["got"], c_s, c_r)
    for m in order:
        for n, copy in c_copies:
            if n == m:
                copy.wait_recv()
        summed = total[m, :16]
        for step in range(3):
            summed = summed + got_c["got"][m, step].astype(jnp.float32)
        out[:, m * HALF : (m + 1) * HALF] = summed.astype(jnp.bfloat16)
    for copy in core_copies[-SLOTS:]:
        copy.wait_send()
    for _, copy in sends + b_copies + c_copies:
        copy.wait_send()


def exchange(a, by_h, rhs, number):
    def dma(*shape):
        return pltpu.SemaphoreType.DMA(shape)

    bf16, f32 = jnp.bfloat16, jnp.float32
    return pl.pallas_call(
        exchange_kernel,
        out_shape=jax.ShapeDtypeStruct((16, 3 * HALF), bf16),
        in_specs=[pl.BlockSpec(memory_space=pl.ANY)] * 5,
        out_specs=pl.BlockSpec(memory_space=pltpu.VMEM),
        scratch_shapes=[
            pltpu.VMEM((3, D, TOKENS), bf16),
            pltpu.VMEM((3, TOKENS, FF), bf16),
            pltpu.VMEM((SLOTS, 256, HALF), bf16),
            pltpu.VMEM((12, 256, HALF), bf16),
            pltpu.VMEM((3, 3, 256, HALF), bf16),
            {"send": pltpu.VMEM((3, 256, HALF), bf16), "got": pltpu.VMEM((3, 3, 64, HALF), bf16)},
            {"send": pltpu.VMEM((3, 64, HALF), bf16), "got": pltpu.VMEM((3, 3, 16, HALF), bf16)},
            pltpu.VMEM((3, 256, HALF), f32),
            dma(11),
            dma(12),
            dma(12),
            *[dma(3, 3)] * 6,
        ],
        compiler_params=pltpu.CompilerParams(collective_id=number, has_side_effects=True, vmem_limit_bytes=67_043_328),
        cost_estimate=pl.CostEstimate(flops=6 * D * TOKENS * FF, bytes_accessed=26_000_000, transcendentals=0),
        name=f"exchange_{number}",
    )(a, by_h, *rhs)


def update(w, m, v, g):
    m = 0.9 * m + 0.1 * g
    v = 0.95 * v + 0.05 * g * g
    step = m * lax.rsqrt(v + 1e-8) + 0.1 * w
    return w - 0.02 * step, m, v


ROWS = 128
STEPS = (D // ROWS, D // ROWS, FF // 256)


def adamw_kernel(*refs):
    g, w, m, v = (refs[i : i + 3] for i in (0, 3, 6, 9))
    new_w, new_m, new_v = refs[-9:-6], refs[-6:-3], refs[-3:]
    i = pl.program_id(0)
    start = 0
    for n in range(3):

        @pl.when((i >= start) & (i < start + STEPS[n]))
        def _(n=n):
            if n < 2:
                parts = [((0, slice(None), slice(half * HALF, (half + 1) * HALF)), g[n][:, half].reshape(ROWS, HALF)) for half in range(2)]
            else:
                parts = [((0, half, 0), g[n][:, half].reshape(D, 128).T) for half in range(2)]
            for at, one in parts:
                a, b, c = update(w[n][at].astype(jnp.float32), m[n][at], v[n][at], one.astype(jnp.float32))
                new_w[n][at] = a.astype(jnp.bfloat16)
                new_m[n][at] = b
                new_v[n][at] = c

        start += STEPS[n]


def adamw(layer, gathered, w, m, v, before):
    def at(n):
        start = sum(STEPS[:n])
        return lambda i: jnp.clip(i - start, 0, STEPS[n] - 1)

    def down(i):
        return 0, 0, 0, 26 + at(2)(i)

    g_specs = [pl.BlockSpec((ROWS // 16, 2, 16, HALF), lambda i, n=n: (at(n)(i), 0, 0, n)) for n in range(2)]
    g_specs.append(pl.BlockSpec((64, 2, 16, 128), down))
    specs = [pl.BlockSpec((1, ROWS, FF), lambda i, n=n: (layer, at(n)(i), 0)) for n in range(2)]
    specs.append(pl.BlockSpec((1, 2, 1, 128, D), lambda i: (layer, 0, at(2)(i), 0, 0)))
    more = [] if before is None else list(before)
    shapes = [jax.ShapeDtypeStruct(one.shape, t) for t in (jnp.bfloat16, jnp.float32, jnp.float32) for one in w]
    return pl.pallas_call(
        adamw_kernel,
        grid=(sum(STEPS),),
        out_shape=shapes,
        in_specs=g_specs + specs * 3 + [pl.BlockSpec(memory_space=pl.ANY)] * len(more),
        out_specs=specs * 3,
        input_output_aliases={12 + i: i for i in range(len(more))},
        compiler_params=pltpu.CompilerParams(vmem_limit_bytes=64_000_000),
        cost_estimate=pl.CostEstimate(flops=60 * D * FF, bytes_accessed=66 * D * FF, transcendentals=3 * D * FF),
        name=f"adamw_{layer}",
    )(gathered, gathered, gathered, *w, *m, *v, *more)


def solution(mesh):
    def step(x, dy, *arrays):
        weights, m, v = (arrays[i : i + 3] for i in (0, 3, 6))
        w_gate, w_up, w_down = weights
        states, by_y = x[0], dy[0]
        gate, up, hidden, a, middle, b = over_hidden(forward_kernel, "forward", 0, "sccr", "fftsss", 1, 3, states, w_gate, w_up, w_down)
        last_hidden, by_gate, by_up = over_hidden(last_layer_kernel, "last_layer", 1, "ssccr", "ttt", 0, 3, by_y, b, w_gate, w_up, w_down)

        def sums(number, a, by_h, *rhs):
            chunk = exchange(a, by_h, rhs, number)
            return lax.all_gather(chunk, "dp", axis=0, tiled=False).reshape(64, 2, 16, 3 * HALF)

        gathered = [None, sums(1, b, by_y, by_gate, by_up, last_hidden)]
        _, back = jax.vjp(normed, middle)
        by_middle = by_y + back(matmul_t(by_gate, w_gate[1]) + matmul_t(by_up, w_up[1]))[0]
        _, by_gate, by_up = by_gate_and_up(gate, up, dot_t(by_middle, w_down[0]))
        gathered[0] = sums(0, a, by_middle, by_gate, by_up, hidden)
        new = None
        split = [(*one[:2], one[2].reshape(2, 2, FF // 256, 128, D)) for one in (weights, m, v)]
        for n in (1, 0):
            new = adamw(n, gathered[n], *split, new)
        return tuple(one.reshape(2, *one.shape[-2:]) if one.ndim == 3 else one.reshape(2, FF, D) for one in new)

    return jax.shard_map(
        step,
        mesh=mesh,
        in_specs=(P(("rep", "dp"), None, None),) * 2 + (P(None, None, None),) * 9,
        out_specs=(P("rep", None, None),) * 9,
        check_vma=False,
    )
```
